32 devices in a mesh: groups: 2 (over y), row: 8 (over z, x), col: 2 (over core).
Axes of the slice: x: 2, y: 2, z: 4, core: 2. Of those that a mesh axis runs over, the one named last changes fastest.
Arguments:
- pair_act: bfloat16 [64, 32, 128], P(('groups', 'row'), 'col'), parts along dimension 0, may hold values from -6 to 6
- in_gain: float32 [128], replicated, may hold values from 0.5 to 1.5
- in_shift: float32 [128], replicated, may hold values from -1 to 1
- left_weight: bfloat16 [128, 256], replicated, may hold values from -0.5 to 0.5
- left_bias: float32 [256], replicated, may hold values from -3 to 3
- right_weight: bfloat16 [128, 256], replicated, may hold values from -0.5 to 0.5
- right_bias: float32 [256], replicated, may hold values from -3 to 3
- gate_weight: bfloat16 [128, 128], replicated, may hold values from -0.5 to 0.5
- gate_bias: float32 [128], replicated, may hold values from -4 to 4
- out_gain: float32 [128], replicated, may hold values from 0.8 to 1.2
- out_shift: float32 [128], replicated, may hold values from -3 to 3
- out_weight: bfloat16 [128, 128], replicated, may hold values from -1 to 1
- out_bias: float32 [128], replicated, may hold values from -3 to 3
Outputs:
- update: bfloat16 [64, 32, 128], P(('groups', 'row'), 'col'), parts along dimension 0
The draws below stay inside these ranges and needn't reach their ends.
There are 2 independent parts, one for each index of `groups`. The reference program is written for one: setup_inputs(seed, part) draws one part's arguments, and reference() takes and returns one part's arrays. A program takes and returns all parts, laid end to end along the dimension named above; an argument that names none is the same for every part. Nothing has to cross between parts.
All inputs are finite; a program needn't handle non-finite values.
Results may differ from the reference program's by a relative error of at most 0.0061.
Values may be sent and summed in bfloat16 or wider, within the bound.
A program may use at most 64 MiB of HBM per device.

```python
import jax
import jax.numpy as jnp
from jax import lax

CZ = 128
CH = 128
N = 32


def bias_halves(base_key):
    gate_key, value_key = jax.random.split(base_key)
    gate_part = jnp.clip(0.7 * jax.random.normal(gate_key, (CH,), jnp.float32), -3.0, 3.0)
    value_part = jnp.clip(0.15 * jax.random.normal(value_key, (CH,), jnp.float32), -0.3, 0.3)
    return jnp.concatenate([gate_part, value_part], axis=0)


def draw_left_bias(key, part):
    return bias_halves(jax.random.fold_in(key, 11))


def draw_right_bias(key, part):
    return bias_halves(jax.random.fold_in(key, 12))


def draw_out_weight(key, part):
    inner_key = jax.random.fold_in(key, 13)
    raw_rows = jnp.clip(jax.random.normal(inner_key, (CH, CZ), jnp.float32), -4.0, 4.0)
    row_norms = jnp.sqrt(jnp.sum(raw_rows * raw_rows, axis=1, keepdims=True) + 1e-06)
    scaled = raw_rows / row_norms
    return scaled.astype(jnp.bfloat16)


def level_of(stream_key, shape, pieces, low, top_value):
    level, own = 1.0, jax.random.fold_in(stream_key, 6)
    for axis_at, shards_of in pieces:
        steps = jnp.exp(jax.random.uniform(jax.random.fold_in(own, axis_at), (shards_of,), jnp.float32, low / len(pieces), top_value / len(pieces)))
        level = level * jnp.repeat(steps, shape[axis_at] // shards_of).reshape([-1 if axis == axis_at else 1 for axis in range(len(shape))])
    return level


def centred(stream_key, shape, deviation, reach, cuts=(), held_as=jnp.bfloat16):
    array = jax.random.normal(stream_key, shape, jnp.float32) * deviation
    if len(cuts) > 0:
        array = level_of(stream_key, shape, cuts, -0.22, 0.18) * array
    return jnp.clip(array, min=-reach, max=reach).astype(held_as)


def setup_inputs(seed: int = 0, part: int = 0) -> dict:
    seeds = jax.random.split(jax.random.key(seed), 14)
    own_keys = jax.random.split(jax.random.fold_in(seeds[13], part), 14)
    pair_act = centred(own_keys[0], (N, N, CZ), 1.0, 6.0, ((0, 8), (1, 2)))
    in_gain = jnp.clip(jax.random.uniform(seeds[1], (CZ,), jnp.float32, 0.5, 1.5), 0.5, 1.5)
    in_shift = centred(seeds[2], (CZ,), 0.2, 1.0, (), jnp.float32)
    left_weight = centred(seeds[3], (CZ, 2 * CH), CZ ** -0.5, 0.5)
    left_bias = draw_left_bias(jax.random.fold_in(seeds[13], 71), part)
    right_weight = centred(seeds[5], (CZ, 2 * CH), CZ ** -0.5, 0.5)
    right_bias = draw_right_bias(jax.random.fold_in(seeds[13], 71), part)
    gate_weight = centred(seeds[7], (CZ, CZ), CZ ** -0.5, 0.5)
    gate_bias = centred(seeds[8], (CZ,), 1.0, 4.0, (), jnp.float32)
    out_gain = jnp.clip(jax.random.uniform(seeds[9], (CH,), jnp.float32, 0.8, 1.2), 0.8, 1.2)
    out_shift = centred(seeds[10], (CH,), 0.5, 3.0, (), jnp.float32)
    out_weight = draw_out_weight(jax.random.fold_in(seeds[13], 71), part)
    out_bias = centred(seeds[12], (CZ,), 0.5, 3.0, (), jnp.float32)
    return dict(pair_act=pair_act, in_gain=in_gain, in_shift=in_shift, left_weight=left_weight, left_bias=left_bias, right_weight=right_weight, right_bias=right_bias, gate_weight=gate_weight, gate_bias=gate_bias, out_gain=out_gain, out_shift=out_shift, out_weight=out_weight, out_bias=out_bias)


def layer_norm(values, gain, shift, axis):
    center = values - lax.optimization_barrier(jnp.mean(values, axis=axis, keepdims=True))
    spread = lax.optimization_barrier(jnp.mean(center * center, axis=axis, keepdims=True))
    return center * lax.rsqrt(spread + 1e-05) * gain + shift

def edge_projection(flat, weight, bias, hidden):
    joined = jnp.dot(flat, weight, preferred_element_type=jnp.float32) + bias
    return (jax.nn.sigmoid(joined[:, :hidden]) * joined[:, hidden:]).astype(jnp.bfloat16)

def channel_product(operands):
    return jnp.dot(operands[0], operands[1].T, preferred_element_type=jnp.float32).astype(jnp.bfloat16)

def reference(pair_act, in_gain, in_shift, left_weight, left_bias, right_weight, right_bias, gate_weight, gate_bias, out_gain, out_shift, out_weight, out_bias):
    length = pair_act.shape[0]
    chans = pair_act.shape[2]
    hidden = left_weight.shape[1] // 2
    normed = layer_norm(pair_act.astype(jnp.float32), in_gain, in_shift, 2).astype(jnp.bfloat16)
    flat = normed.reshape(length * length, chans)
    left_edge = edge_projection(flat, left_weight, left_bias, hidden)
    right_edge = edge_projection(flat, right_weight, right_bias, hidden)
    gate = jax.nn.sigmoid(jnp.dot(flat, gate_weight, preferred_element_type=jnp.float32) + gate_bias)
    left_chan = left_edge.reshape(length, length, hidden).transpose(2, 0, 1)
    right_chan = right_edge.reshape(length, length, hidden).transpose(2, 0, 1)
    triangle = lax.map(channel_product, (left_chan, right_chan))
    triangle_flat = triangle.transpose(1, 2, 0).reshape(length * length, hidden)
    mixed = layer_norm(triangle_flat.astype(jnp.float32), out_gain, out_shift, 1).astype(jnp.bfloat16)
    projected = jnp.dot(mixed, out_weight, preferred_element_type=jnp.float32) + out_bias
    update = (gate * projected).astype(jnp.bfloat16)
    return update.reshape(length, length, chans)
```

```python
import functools

import jax
import jax.numpy as jnp
from jax import lax
from jax.experimental import pallas as pl
from jax.experimental.pallas import tpu as pltpu
from jax.sharding import PartitionSpec as P

MESH = pl.DeviceIdType.MESH
KERNEL_BYTES = 2 * 1024 * 1024


def layer_norm(values, gain, shift, axis):
    center = values - jnp.mean(values, axis=axis, keepdims=True)
    spread = jnp.mean(center * center, axis=axis, keepdims=True)
    return center * lax.rsqrt(spread + 1e-05) * gain + shift


def edge_projection(normed, weight, bias, hidden):
    joined = (
        jnp.einsum("rkc,cd->drk", normed, weight, preferred_element_type=jnp.float32)
        + bias[:, None, None]
    )
    return (jax.nn.sigmoid(joined[:hidden]) * joined[hidden:]).astype(jnp.bfloat16)


def collective_plan(
    pair_act,
    in_gain,
    in_shift,
    left_weight,
    left_bias,
    right_weight,
    right_bias,
    gate_weight,
    gate_bias,
    out_gain,
    out_shift,
    out_weight,
    out_bias,
):
    hidden = left_weight.shape[1] // 2
    normed = layer_norm(pair_act.astype(jnp.float32), in_gain, in_shift, 2).astype(jnp.bfloat16)
    left_edge = edge_projection(normed, left_weight, left_bias, hidden)
    right_edge = edge_projection(normed, right_weight, right_bias, hidden)
    gate = jax.nn.sigmoid(
        jnp.einsum("rkc,cd->rkd", normed, gate_weight, preferred_element_type=jnp.float32)
        + gate_bias
    )
    left_chan, right_chan = (
        lax.all_to_all(left_edge, "row", split_axis=0, concat_axis=1, tiled=True),
        lax.all_to_all(right_edge, "row", split_axis=0, concat_axis=1, tiled=True),
    )
    left_full = lax.all_gather(left_chan, "col", axis=2, tiled=True)
    right_mine = lax.all_to_all(right_chan, "col", split_axis=1, concat_axis=2, tiled=True)
    summed = jnp.einsum("cik,cjk->cij", left_full, right_mine, preferred_element_type=jnp.float32)
    triangle_chan = summed.astype(jnp.bfloat16)
    triangle = lax.all_to_all(triangle_chan, "row", split_axis=1, concat_axis=0, tiled=True)
    mixed = layer_norm(
        triangle.astype(jnp.float32), out_gain[:, None, None], out_shift[:, None, None], 0
    ).astype(jnp.bfloat16)
    projected = (
        jnp.einsum("cij,cd->ijd", mixed, out_weight, preferred_element_type=jnp.float32) + out_bias
    )
    return (gate * projected).astype(jnp.bfloat16)


def kernel(n_row, n_col, *refs):
    sources, out_ref, held, rest = refs[:13], refs[13], refs[14:27], refs[27:]
    (right_own, right_all, left_all, partial, load_sem, left_sems, right_send, right_recv) = rest
    (pair, in_gain, in_shift, left_w, left_b, right_w, right_b) = held[:7]
    (gate_w, gate_b, out_gain, out_shift, out_w, out_b) = held[7:]
    row, col = lax.axis_index("row"), lax.axis_index("col")
    span = n_row // n_col
    rows, cols, chans = pair.shape
    hidden = left_w.shape[1] // 2
    others = [lax.rem(col + step, n_col) for step in range(1, n_col)]
    target_col, slot = row // span, lax.rem(row, span)

    barrier = pltpu.get_barrier_semaphore()
    for step in range(span):
        for from_col in range(n_col):
            from_row = col * span + step

            @pl.when(jnp.logical_or(from_row != row, from_col != col))
            def _():
                pl.semaphore_signal(
                    barrier, 1, device_id={"row": from_row, "col": from_col}, device_id_type=MESH
                )
    for other in others:
        pl.semaphore_signal(barrier, 1, device_id={"col": other}, device_id_type=MESH)

    loads = [
        pltpu.make_async_copy(src, dst, load_sem.at[at])
        for at, (src, dst) in enumerate(zip(sources, held))
    ]
    for load in loads:
        load.start()

    def edges(weight, bias):
        joined = jnp.dot(normed, weight[...], preferred_element_type=jnp.float32) + bias[...]
        edge = jax.nn.sigmoid(joined[:, :hidden]) * joined[:, hidden:]
        return edge.astype(jnp.bfloat16).reshape(rows, cols, hidden)

    for at in (0, 1, 2):
        loads[at].wait()
    values = pair[...].astype(jnp.float32).reshape(rows * cols, chans)
    normed = layer_norm(values, in_gain[...], in_shift[...], 1).astype(jnp.bfloat16)
    for at in (5, 6):
        loads[at].wait()
    right_edge = edges(right_w, right_b)
    right_own[...] = right_edge

    @pl.when(target_col == col)
    def _():
        right_all[slot, col] = right_edge

    for at in (3, 4):
        loads[at].wait()
    left_all[col] = edges(left_w, left_b)

    own = (target_col == col).astype(jnp.int32)
    pl.semaphore_wait(barrier, n_row - own + n_col - 1)

    right_copies = []
    for step in range(n_row):
        to_row = lax.rem(row + n_row // 2 + step, n_row)
        copy = pltpu.make_async_remote_copy(
            src_ref=right_own,
            dst_ref=right_all.at[slot, col],
            send_sem=right_send.at[step],
            recv_sem=right_recv.at[slot, col],
            device_id={"row": to_row, "col": target_col},
            device_id_type=MESH,
        )
        remote = jnp.logical_or(to_row != row, target_col != col)
        right_copies.append((copy, remote))
        pl.when(remote)(copy.start)
    left_copies = []
    for step, other in enumerate(others):
        copy = pltpu.make_async_remote_copy(
            src_ref=left_all.at[col],
            dst_ref=left_all.at[col],
            send_sem=left_sems.at[0, step],
            recv_sem=left_sems.at[1, step],
            device_id={"col": other},
            device_id_type=MESH,
        )
        left_copies.append(copy)
        copy.start()

    for at in (7, 8, 9, 10, 11, 12):
        loads[at].wait()
    gate = jax.nn.sigmoid(
        jnp.dot(normed, gate_w[...], preferred_element_type=jnp.float32) + gate_b[...]
    )

    for copy in left_copies:
        copy.wait_recv()
    left = [left_all[part].astype(jnp.float32) for part in range(n_col)]
    for step in range(span):
        for part in range(n_col):
            from_row = col * span + step

            @pl.when(jnp.logical_or(from_row != row, part != col))
            def _():
                pltpu.make_async_remote_copy(
                    src_ref=right_own,
                    dst_ref=right_all.at[step, part],
                    send_sem=right_send.at[0],
                    recv_sem=right_recv.at[step, part],
                    device_id={"row": from_row, "col": part},
                    device_id_type=MESH,
                ).wait_recv()

    for step in range(span):
        for j in range(rows):
            right = [right_all[step, part, j].astype(jnp.float32) for part in range(n_col)]
            for i in range(rows):
                product = sum(left[part][i] * right[part] for part in range(n_col))
                product = product.reshape(cols // 8, 8, hidden).sum(axis=0)
                partial[pl.ds(((i * span + step) * rows + j) * 8, 8), :] = product
    n_pairs = rows * span * rows
    triangle = sum(partial[pl.ds(at, n_pairs, stride=8), :] for at in range(8))
    triangle = triangle.astype(jnp.bfloat16).astype(jnp.float32)
    mixed = layer_norm(triangle, out_gain[...], out_shift[...], 1).astype(jnp.bfloat16)
    projected = jnp.dot(mixed, out_w[...], preferred_element_type=jnp.float32) + out_b[...]
    out_ref[...] = (gate * projected).astype(jnp.bfloat16).reshape(out_ref.shape)

    for copy, remote in right_copies:
        pl.when(remote)(copy.wait_send)
    for copy in left_copies:
        copy.wait_send()


def kernel_plan(n_row, n_col, pair_act, *params):
    rows, cols, chans = pair_act.shape
    hidden = params[2].shape[1] // 2
    span = n_row // n_col
    operands = [pair_act] + [p.reshape(1, -1) if p.ndim == 1 else p for p in params]
    scratch = [pltpu.VMEM(o.shape, o.dtype) for o in operands]
    scratch += [
        pltpu.VMEM((rows, cols, hidden), jnp.bfloat16),
        pltpu.VMEM((span, n_col, rows, cols, hidden), jnp.bfloat16),
        pltpu.VMEM((n_col, rows, cols, hidden), jnp.bfloat16),
        pltpu.VMEM((rows * span * rows * 8, hidden), jnp.float32),
        pltpu.SemaphoreType.DMA((len(operands),)),
        pltpu.SemaphoreType.DMA((2, max(n_col - 1, 1))),
        pltpu.SemaphoreType.DMA((n_row,)),
        pltpu.SemaphoreType.DMA((span, n_col)),
    ]
    return pl.pallas_call(
        functools.partial(kernel, n_row, n_col),
        out_shape=jax.ShapeDtypeStruct((rows, cols, chans), jnp.bfloat16),
        in_specs=[pl.BlockSpec(memory_space=pl.ANY)] * len(operands),
        out_specs=pl.BlockSpec(memory_space=pltpu.VMEM),
        scratch_shapes=scratch,
        compiler_params=pltpu.CompilerParams(collective_id=0, has_side_effects=True),
    )(*operands)


def fits(n_row, n_col, rows, cols, hidden):
    gathered = n_row * rows * cols * hidden * 2
    square = rows * n_row == cols * n_col
    return square and n_row % n_col == 0 and cols % 8 == 0 and gathered <= KERNEL_BYTES


def solution(mesh):
    n_row, n_col = mesh.shape["row"], mesh.shape["col"]

    def per_device(pair_act, *params):
        rows, cols, _ = pair_act.shape
        if fits(n_row, n_col, rows, cols, params[2].shape[1] // 2):
            return kernel_plan(n_row, n_col, pair_act, *params)
        return collective_plan(pair_act, *params)

    spec = P(("groups", "row"), "col", None)
    return jax.shard_map(
        per_device, mesh=mesh, in_specs=(spec,) + (P(),) * 12, out_specs=spec, check_vma=False
    )
```

```python
import functools

import jax
import jax.numpy as jnp
from jax import lax
from jax.experimental import pallas as pl
from jax.experimental.pallas import tpu as pltpu
from jax.sharding import PartitionSpec as P

MESH = pl.DeviceIdType.MESH
KERNEL_BYTES = 2 * 1024 * 1024


def layer_norm(values, gain, shift, axis):
    center = values - jnp.mean(values, axis=axis, keepdims=True)
    spread = jnp.mean(center * center, axis=axis, keepdims=True)
    return center * lax.rsqrt(spread + 1e-05) * gain + shift


def edge_projection(normed, weight, bias, hidden):
    joined = (
        jnp.einsum("rkc,cd->drk", normed, weight, preferred_element_type=jnp.float32)
        + bias[:, None, None]
    )
    return (jax.nn.sigmoid(joined[:hidden]) * joined[hidden:]).astype(jnp.bfloat16)


def collective_plan(
    pair_act,
    in_gain,
    in_shift,
    left_weight,
    left_bias,
    right_weight,
    right_bias,
    gate_weight,
    gate_bias,
    out_gain,
    out_shift,
    out_weight,
    out_bias,
):
    hidden = left_weight.shape[1] // 2
    normed = layer_norm(pair_act.astype(jnp.float32), in_gain, in_shift, 2).astype(jnp.bfloat16)
    left_edge = edge_projection(normed, left_weight, left_bias, hidden)
    right_edge = edge_projection(normed, right_weight, right_bias, hidden)
    gate = jax.nn.sigmoid(
        jnp.einsum("rkc,cd->rkd", normed, gate_weight, preferred_element_type=jnp.float32)
        + gate_bias
    )
    left_chan, right_chan = (
        lax.all_to_all(left_edge, "row", split_axis=0, concat_axis=1, tiled=True),
        lax.all_to_all(right_edge, "row", split_axis=0, concat_axis=1, tiled=True),
    )
    left_full = lax.all_gather(left_chan, "col", axis=2, tiled=True)
    right_mine = lax.all_to_all(right_chan, "col", split_axis=1, concat_axis=2, tiled=True)
    summed = jnp.einsum("cik,cjk->cij", left_full, right_mine, preferred_element_type=jnp.float32)
    triangle_chan = summed.astype(jnp.bfloat16)
    triangle = lax.all_to_all(triangle_chan, "row", split_axis=1, concat_axis=0, tiled=True)
    mixed = layer_norm(
        triangle.astype(jnp.float32), out_gain[:, None, None], out_shift[:, None, None], 0
    ).astype(jnp.bfloat16)
    projected = (
        jnp.einsum("cij,cd->ijd", mixed, out_weight, preferred_element_type=jnp.float32) + out_bias
    )
    return (gate * projected).astype(jnp.bfloat16)


def kernel(n_row, n_col, *refs):
    sources, out_ref, held, rest = refs[:13], refs[13], refs[14:27], refs[27:]
    (right_own, right_all, left_all, partial, load_sem, left_sems, right_send, right_recv) = rest
    (pair, in_gain, in_shift, left_w, left_b, right_w, right_b) = held[:7]
    (gate_w, gate_b, out_gain, out_shift, out_w, out_b) = held[7:]
    row, col = lax.axis_index("row"), lax.axis_index("col")
    span = n_row // n_col
    rows, cols, chans = pair.shape
    hidden = left_w.shape[1] // 2
    others = [lax.rem(col + step, n_col) for step in range(1, n_col)]
    target_col, slot = row // span, lax.rem(row, span)

    barrier = pltpu.get_barrier_semaphore()
    for step in range(span):
        for from_col in range(n_col):
            from_row = col * span + step

            @pl.when(jnp.logical_or(from_row != row, from_col != col))
            def _():
                pl.semaphore_signal(
                    barrier, 1, device_id={"row": from_row, "col": from_col}, device_id_type=MESH
                )
    for other in others:
        pl.semaphore_signal(barrier, 1, device_id={"col": other}, device_id_type=MESH)

    loads = [
        pltpu.make_async_copy(src, dst, load_sem.at[at])
        for at, (src, dst) in enumerate(zip(sources, held))
    ]
    for load in loads:
        load.start()

    def edges(weight, bias):
        joined = jnp.dot(normed, weight[...], preferred_element_type=jnp.float32) + bias[...]
        edge = jax.nn.sigmoid(joined[:, :hidden]) * joined[:, hidden:]
        return edge.astype(jnp.bfloat16).reshape(rows, cols, hidden)

    for at in (0, 1, 2):
        loads[at].wait()
    values = pair[...].astype(jnp.float32).reshape(rows * cols, chans)
    normed = layer_norm(values, in_gain[...], in_shift[...], 1).astype(jnp.bfloat16)
    for at in (5, 6):
        loads[at].wait()
    right_edge = edges(right_w, right_b)
    right_own[...] = right_edge

    @pl.when(target_col == col)
    def _():
        right_all[slot, col] = right_edge

    for at in (3, 4):
        loads[at].wait()
    left_all[col] = edges(left_w, left_b)

    own = (target_col == col).astype(jnp.int32)
    pl.semaphore_wait(barrier, n_row - own + n_col - 1)

    right_copies = []
    for step in range(n_row):
        above = n_row - 1 - row
        to_row = jnp.where(step < above, n_row - 1 - step, step - above)
        copy = pltpu.make_async_remote_copy(
            src_ref=right_own,
            dst_ref=right_all.at[slot, col],
            send_sem=right_send.at[step],
            recv_sem=right_recv.at[slot, col],
            device_id={"row": to_row, "col": target_col},
            device_id_type=MESH,
        )
        remote = jnp.logical_or(to_row != row, target_col != col)
        right_copies.append((copy, remote))
        pl.when(remote)(copy.start)
    left_copies = []
    for step, other in enumerate(others):
        copy = pltpu.make_async_remote_copy(
            src_ref=left_all.at[col],
            dst_ref=left_all.at[col],
            send_sem=left_sems.at[0, step],
            recv_sem=left_sems.at[1, step],
            device_id={"col": other},
            device_id_type=MESH,
        )
        left_copies.append(copy)
        copy.start()

    for at in (7, 8, 9, 10, 11, 12):
        loads[at].wait()
    gate = jax.nn.sigmoid(
        jnp.dot(normed, gate_w[...], preferred_element_type=jnp.float32) + gate_b[...]
    )

    for copy in left_copies:
        copy.wait_recv()
    left = [left_all[part].astype(jnp.float32) for part in range(n_col)]
    backwards = (row > col * span).astype(jnp.int32)
    for step in range(span):
        block = step + backwards * (span - 1 - 2 * step)
        for part in range(n_col):

            @pl.when(jnp.logical_or(col * span + block != row, part != col))
            def _():
                pltpu.make_async_remote_copy(
                    src_ref=right_own,
                    dst_ref=right_all.at[block, part],
                    send_sem=right_send.at[0],
                    recv_sem=right_recv.at[block, part],
                    device_id={"row": col * span + block, "col": part},
                    device_id_type=MESH,
                ).wait_recv()

        for j in range(rows):
            right = [right_all[block, part, j].astype(jnp.float32) for part in range(n_col)]
            for i in range(rows):
                product = sum(left[part][i] * right[part] for part in range(n_col))
                product = product.reshape(cols // 8, 8, hidden).sum(axis=0)
                at = pl.multiple_of(((i * span + block) * rows + j) * 8, 8)
                partial[pl.ds(at, 8), :] = product
    n_pairs = rows * span * rows
    triangle = sum(partial[pl.ds(at, n_pairs, stride=8), :] for at in range(8))
    triangle = triangle.astype(jnp.bfloat16).astype(jnp.float32)
    mixed = layer_norm(triangle, out_gain[...], out_shift[...], 1).astype(jnp.bfloat16)
    projected = jnp.dot(mixed, out_w[...], preferred_element_type=jnp.float32) + out_b[...]
    out_ref[...] = (gate * projected).astype(jnp.bfloat16).reshape(out_ref.shape)

    for copy, remote in right_copies:
        pl.when(remote)(copy.wait_send)
    for copy in left_copies:
        copy.wait_send()


def kernel_plan(n_row, n_col, pair_act, *params):
    rows, cols, chans = pair_act.shape
    hidden = params[2].shape[1] // 2
    span = n_row // n_col
    operands = [pair_act] + [p.reshape(1, -1) if p.ndim == 1 else p for p in params]
    scratch = [pltpu.VMEM(o.shape, o.dtype) for o in operands]
    scratch += [
        pltpu.VMEM((rows, cols, hidden), jnp.bfloat16),
        pltpu.VMEM((span, n_col, rows, cols, hidden), jnp.bfloat16),
        pltpu.VMEM((n_col, rows, cols, hidden), jnp.bfloat16),
        pltpu.VMEM((rows * span * rows * 8, hidden), jnp.float32),
        pltpu.SemaphoreType.DMA((len(operands),)),
        pltpu.SemaphoreType.DMA((2, max(n_col - 1, 1))),
        pltpu.SemaphoreType.DMA((n_row,)),
        pltpu.SemaphoreType.DMA((span, n_col)),
    ]
    return pl.pallas_call(
        functools.partial(kernel, n_row, n_col),
        out_shape=pltpu.VMEM((rows, cols, chans), jnp.bfloat16),
        in_specs=[pl.BlockSpec(memory_space=pl.ANY)] * len(operands),
        out_specs=pl.BlockSpec(memory_space=pltpu.VMEM),
        scratch_shapes=scratch,
        compiler_params=pltpu.CompilerParams(collective_id=0, has_side_effects=True),
    )(*operands)


def fits(n_row, n_col, rows, cols, hidden):
    gathered = n_row * rows * cols * hidden * 2
    square = rows * n_row == cols * n_col
    return square and n_row % n_col == 0 and cols % 8 == 0 and gathered <= KERNEL_BYTES


def solution(mesh):
    n_row, n_col = mesh.shape["row"], mesh.shape["col"]

    def per_device(pair_act, *params):
        rows, cols, _ = pair_act.shape
        if fits(n_row, n_col, rows, cols, params[2].shape[1] // 2):
            return kernel_plan(n_row, n_col, pair_act, *params)
        return collective_plan(pair_act, *params)

    spec = P(("groups", "row"), "col", None)
    return jax.shard_map(
        per_device, mesh=mesh, in_specs=(spec,) + (P(),) * 12, out_specs=spec, check_vma=False
    )
```

```python
import functools

import jax
import jax.numpy as jnp
from jax import lax
from jax.experimental import pallas as pl
from jax.experimental.pallas import tpu as pltpu
from jax.sharding import PartitionSpec as P

MESH = pl.DeviceIdType.MESH
KERNEL_BYTES = 2 * 1024 * 1024


def layer_norm(values, gain, shift, axis):
    center = values - jnp.mean(values, axis=axis, keepdims=True)
    spread = jnp.mean(center * center, axis=axis, keepdims=True)
    return center * lax.rsqrt(spread + 1e-05) * gain + shift


def edge_projection(normed, weight, bias, hidden):
    joined = (
        jnp.einsum("rkc,cd->drk", normed, weight, preferred_element_type=jnp.float32)
        + bias[:, None, None]
    )
    return (jax.nn.sigmoid(joined[:hidden]) * joined[hidden:]).astype(jnp.bfloat16)


def collective_plan(
    pair_act,
    in_gain,
    in_shift,
    left_weight,
    left_bias,
    right_weight,
    right_bias,
    gate_weight,
    gate_bias,
    out_gain,
    out_shift,
    out_weight,
    out_bias,
):
    hidden = left_weight.shape[1] // 2
    normed = layer_norm(pair_act.astype(jnp.float32), in_gain, in_shift, 2).astype(jnp.bfloat16)
    left_edge = edge_projection(normed, left_weight, left_bias, hidden)
    right_edge = edge_projection(normed, right_weight, right_bias, hidden)
    gate = jax.nn.sigmoid(
        jnp.einsum("rkc,cd->rkd", normed, gate_weight, preferred_element_type=jnp.float32)
        + gate_bias
    )
    left_chan, right_chan = (
        lax.all_to_all(left_edge, "row", split_axis=0, concat_axis=1, tiled=True),
        lax.all_to_all(right_edge, "row", split_axis=0, concat_axis=1, tiled=True),
    )
    left_full = lax.all_gather(left_chan, "col", axis=2, tiled=True)
    right_mine = lax.all_to_all(right_chan, "col", split_axis=1, concat_axis=2, tiled=True)
    summed = jnp.einsum("cik,cjk->cij", left_full, right_mine, preferred_element_type=jnp.float32)
    triangle_chan = summed.astype(jnp.bfloat16)
    triangle = lax.all_to_all(triangle_chan, "row", split_axis=1, concat_axis=0, tiled=True)
    mixed = layer_norm(
        triangle.astype(jnp.float32), out_gain[:, None, None], out_shift[:, None, None], 0
    ).astype(jnp.bfloat16)
    projected = (
        jnp.einsum("cij,cd->ijd", mixed, out_weight, preferred_element_type=jnp.float32) + out_bias
    )
    return (gate * projected).astype(jnp.bfloat16)


def sigmoid(values):
    return 0.5 * jnp.tanh(0.5 * values) + 0.5


def kernel(n_row, n_col, *refs):
    sources, out_ref, held, rest = refs[:13], refs[13], refs[14:27], refs[27:]
    (right_own, right_all, left_all, partial, load_sem, left_sems, right_send, right_recv, ready) = rest
    (pair, in_gain, in_shift, left_w, left_b, right_w, right_b) = held[:7]
    (gate_w, gate_b, out_gain, out_shift, out_w, out_b) = held[7:]
    row, col = lax.axis_index("row"), lax.axis_index("col")
    span = n_row // n_col
    rows, cols, chans = pair.shape
    hidden = left_w.shape[1] // 2
    others = [lax.rem(col + step, n_col) for step in range(1, n_col)]
    target_col, slot = row // span, lax.rem(row, span)

    own = (target_col == col).astype(jnp.int32)

    loads = [
        pltpu.make_async_copy(src, dst, load_sem.at[at])
        for at, (src, dst) in enumerate(zip(sources, held))
    ]
    for at in (0, 1, 2, 5, 6, 3, 4, 7, 8, 9, 10, 11, 12):
        loads[at].start()

    barrier = pltpu.get_barrier_semaphore()
    for step in range(span):
        for from_col in range(n_col):
            from_row = col * span + step
            remote = jnp.logical_or(from_row != row, from_col != col)

            @pl.when(jnp.logical_and(from_row >= row, remote))
            def _():
                pl.semaphore_signal(
                    barrier, 1, device_id={"row": from_row, "col": from_col}, device_id_type=MESH
                )
    for to_row in range(1, n_row):

        @pl.when(to_row > row)
        def _():
            pl.semaphore_signal(
                barrier, 1, device_id={"row": to_row, "col": target_col}, device_id_type=MESH
            )
    for other in others:
        pl.semaphore_signal(barrier, 1, device_id={"col": other}, device_id_type=MESH)

    earlier = jnp.clip(row - col * span, 0, span)
    pl.semaphore_wait(barrier, row + 1 - own + n_col * earlier + n_col - 1)
    for step in range(span):
        for from_col in range(n_col):
            from_row = col * span + step

            @pl.when(from_row < row)
            def _():
                pl.semaphore_signal(
                    ready.at[row],
                    1,
                    device_id={"row": from_row, "col": from_col},
                    device_id_type=MESH,
                )

    def edges(weight, bias):
        joined = jnp.dot(normed, weight[...], preferred_element_type=jnp.float32) + bias[...]
        edge = sigmoid(joined[:, :hidden]) * joined[:, hidden:]
        return edge.astype(jnp.bfloat16).reshape(rows, cols, hidden)

    for at in (0, 1, 2):
        loads[at].wait()
    values = pair[...].astype(jnp.float32).reshape(rows * cols, chans)
    normed = layer_norm(values, in_gain[...], in_shift[...], 1).astype(jnp.bfloat16)
    for at in (5, 6):
        loads[at].wait()
    right_edge = edges(right_w, right_b)
    right_own[...] = right_edge

    @pl.when(target_col == col)
    def _():
        right_all[slot, col] = right_edge

    def right_copy(to_row):
        return pltpu.make_async_remote_copy(
            src_ref=right_own,
            dst_ref=right_all.at[slot, col],
            send_sem=right_send.at[to_row],
            recv_sem=right_recv.at[slot, col],
            device_id={"row": to_row, "col": target_col},
            device_id_type=MESH,
        )

    for to_row in range(n_row):
        remote = jnp.logical_or(to_row < row, jnp.logical_and(to_row == row, target_col != col))

        @pl.when(remote)
        def _():
            right_copy(to_row).start()

    for at in (3, 4):
        loads[at].wait()
    left_all[col] = edges(left_w, left_b)
    left_copies = []
    for step, other in enumerate(others):
        copy = pltpu.make_async_remote_copy(
            src_ref=left_all.at[col],
            dst_ref=left_all.at[col],
            send_sem=left_sems.at[0, step],
            recv_sem=left_sems.at[1, step],
            device_id={"col": other},
            device_id_type=MESH,
        )
        left_copies.append(copy)
        copy.start()

    for at in (7, 8, 9, 10, 11, 12):
        loads[at].wait()
    gate = sigmoid(
        jnp.dot(normed, gate_w[...], preferred_element_type=jnp.float32) + gate_b[...]
    )

    for to_row in range(1, n_row):

        @pl.when(to_row > row)
        def _():
            pl.semaphore_wait(ready.at[to_row], 1)
            right_copy(to_row).start()

    for copy in left_copies:
        copy.wait_recv()
    left = [left_all[part].astype(jnp.float32) for part in range(n_col)]
    backwards = (row > col * span).astype(jnp.int32)
    for step in range(span):
        block = step + backwards * (span - 1 - 2 * step)
        for part in range(n_col):

            @pl.when(jnp.logical_or(col * span + block != row, part != col))
            def _():
                pltpu.make_async_remote_copy(
                    src_ref=right_own,
                    dst_ref=right_all.at[block, part],
                    send_sem=right_send.at[0],
                    recv_sem=right_recv.at[block, part],
                    device_id={"row": col * span + block, "col": part},
                    device_id_type=MESH,
                ).wait_recv()

        for j in range(rows):
            right = [right_all[block, part, j].astype(jnp.float32) for part in range(n_col)]
            for i in range(rows):
                product = sum(left[part][i] * right[part] for part in range(n_col))
                product = product.reshape(cols // 8, 8, hidden).sum(axis=0)
                at = pl.multiple_of(((i * span + block) * rows + j) * 8, 8)
                partial[pl.ds(at, 8), :] = product
    n_pairs = rows * span * rows
    triangle = sum(partial[pl.ds(at, n_pairs, stride=8), :] for at in range(8))
    triangle = triangle.astype(jnp.bfloat16).astype(jnp.float32)
    mixed = layer_norm(triangle, out_gain[...], out_shift[...], 1).astype(jnp.bfloat16)
    projected = jnp.dot(mixed, out_w[...], preferred_element_type=jnp.float32) + out_b[...]
    out_ref[...] = (gate * projected).astype(jnp.bfloat16).reshape(out_ref.shape)

    for to_row in range(n_row):

        @pl.when(jnp.logical_or(to_row != row, target_col != col))
        def _():
            right_copy(to_row).wait_send()

    for copy in left_copies:
        copy.wait_send()


def kernel_plan(n_row, n_col, pair_act, *params):
    rows, cols, chans = pair_act.shape
    hidden = params[2].shape[1] // 2
    span = n_row // n_col
    operands = [pair_act] + [p.reshape(1, -1) if p.ndim == 1 else p for p in params]
    scratch = [pltpu.VMEM(o.shape, o.dtype) for o in operands]
    scratch += [
        pltpu.VMEM((rows, cols, hidden), jnp.bfloat16),
        pltpu.VMEM((span, n_col, rows, cols, hidden), jnp.bfloat16),
        pltpu.VMEM((n_col, rows, cols, hidden), jnp.bfloat16),
        pltpu.VMEM((rows * span * rows * 8, hidden), jnp.float32),
        pltpu.SemaphoreType.DMA((len(operands),)),
        pltpu.SemaphoreType.DMA((2, max(n_col - 1, 1))),
        pltpu.SemaphoreType.DMA((n_row,)),
        pltpu.SemaphoreType.DMA((span, n_col)),
        pltpu.SemaphoreType.REGULAR((n_row,)),
    ]
    return pl.pallas_call(
        functools.partial(kernel, n_row, n_col),
        out_shape=pltpu.VMEM((rows, cols, chans), jnp.bfloat16),
        in_specs=[pl.BlockSpec(memory_space=pl.ANY)] * len(operands),
        out_specs=pl.BlockSpec(memory_space=pltpu.VMEM),
        scratch_shapes=scratch,
        compiler_params=pltpu.CompilerParams(collective_id=0, has_side_effects=True),
    )(*operands)


def fits(n_row, n_col, rows, cols, hidden):
    gathered = n_row * rows * cols * hidden * 2
    square = rows * n_row == cols * n_col
    return square and n_row % n_col == 0 and cols % 8 == 0 and gathered <= KERNEL_BYTES


def solution(mesh):
    n_row, n_col = mesh.shape["row"], mesh.shape["col"]

    def per_device(pair_act, *params):
        rows, cols, _ = pair_act.shape
        if fits(n_row, n_col, rows, cols, params[2].shape[1] // 2):
            return kernel_plan(n_row, n_col, pair_act, *params)
        return collective_plan(pair_act, *params)

    spec = P(("groups", "row"), "col", None)
    return jax.shard_map(
        per_device, mesh=mesh, in_specs=(spec,) + (P(),) * 12, out_specs=spec, check_vma=False
    )
```

```python
import functools

import jax
import jax.numpy as jnp
from jax import lax
from jax.experimental import pallas as pl
from jax.experimental.pallas import tpu as pltpu
from jax.sharding import PartitionSpec as P

MESH = pl.DeviceIdType.MESH
KERNEL_BYTES = 2 * 1024 * 1024


def layer_norm(values, gain, shift, axis):
    center = values - jnp.mean(values, axis=axis, keepdims=True)
    spread = jnp.mean(center * center, axis=axis, keepdims=True)
    return center * lax.rsqrt(spread + 1e-05) * gain + shift


def edge_projection(normed, weight, bias, hidden):
    joined = (
        jnp.einsum("rkc,cd->drk", normed, weight, preferred_element_type=jnp.float32)
        + bias[:, None, None]
    )
    return (jax.nn.sigmoid(joined[:hidden]) * joined[hidden:]).astype(jnp.bfloat16)


def collective_plan(
    pair_act,
    in_gain,
    in_shift,
    left_weight,
    left_bias,
    right_weight,
    right_bias,
    gate_weight,
    gate_bias,
    out_gain,
    out_shift,
    out_weight,
    out_bias,
):
    hidden = left_weight.shape[1] // 2
    normed = layer_norm(pair_act.astype(jnp.float32), in_gain, in_shift, 2).astype(jnp.bfloat16)
    left_edge = edge_projection(normed, left_weight, left_bias, hidden)
    right_edge = edge_projection(normed, right_weight, right_bias, hidden)
    gate = jax.nn.sigmoid(
        jnp.einsum("rkc,cd->rkd", normed, gate_weight, preferred_element_type=jnp.float32)
        + gate_bias
    )
    left_chan, right_chan = (
        lax.all_to_all(left_edge, "row", split_axis=0, concat_axis=1, tiled=True),
        lax.all_to_all(right_edge, "row", split_axis=0, concat_axis=1, tiled=True),
    )
    left_full = lax.all_gather(left_chan, "col", axis=2, tiled=True)
    right_mine = lax.all_to_all(right_chan, "col", split_axis=1, concat_axis=2, tiled=True)
    summed = jnp.einsum("cik,cjk->cij", left_full, right_mine, preferred_element_type=jnp.float32)
    triangle_chan = summed.astype(jnp.bfloat16)
    triangle = lax.all_to_all(triangle_chan, "row", split_axis=1, concat_axis=0, tiled=True)
    mixed = layer_norm(
        triangle.astype(jnp.float32), out_gain[:, None, None], out_shift[:, None, None], 0
    ).astype(jnp.bfloat16)
    projected = (
        jnp.einsum("cij,cd->ijd", mixed, out_weight, preferred_element_type=jnp.float32) + out_bias
    )
    return (gate * projected).astype(jnp.bfloat16)


def sigmoid(values):
    return 0.5 * jnp.tanh(0.5 * values) + 0.5


def spread_of(center):
    return lax.rsqrt(jnp.mean(center * center, axis=1, keepdims=True) + 1e-05)


def shift_product(shift, weight):
    high = shift.astype(jnp.bfloat16)
    low = (shift - high.astype(jnp.float32)).astype(jnp.bfloat16)
    both = (jnp.broadcast_to(part, (16, part.shape[1])) for part in (high, low))
    return sum(jnp.dot(part, weight, preferred_element_type=jnp.float32) for part in both)[:1]


def kernel(n_row, n_col, *refs):
    sources, out_ref, held, rest = refs[:13], refs[13], refs[14:27], refs[27:]
    (right_own, right_all, left_all, partial, load_sem, left_sems, right_send, right_recv, ready) = rest
    (pair, in_gain, in_shift, left_w, left_b, right_w, right_b) = held[:7]
    (gate_w, gate_b, out_gain, out_shift, out_w, out_b) = held[7:]
    row, col = lax.axis_index("row"), lax.axis_index("col")
    span = n_row // n_col
    rows, cols, chans = pair.shape
    hidden = left_w.shape[1] // 2
    others = [lax.rem(col + step, n_col) for step in range(1, n_col)]
    target_col, slot = row // span, lax.rem(row, span)

    own = (target_col == col).astype(jnp.int32)

    loads = [
        pltpu.make_async_copy(src, dst, load_sem.at[at])
        for at, (src, dst) in enumerate(zip(sources, held))
    ]
    for at in (0, 1, 2, 5, 6, 3, 4, 7, 8, 9, 10, 11, 12):
        loads[at].start()

    barrier = pltpu.get_barrier_semaphore()
    for step in range(span):
        for from_col in range(n_col):
            from_row = col * span + step
            remote = jnp.logical_or(from_row != row, from_col != col)

            @pl.when(jnp.logical_and(from_row >= row, remote))
            def _():
                pl.semaphore_signal(
                    barrier, 1, device_id={"row": from_row, "col": from_col}, device_id_type=MESH
                )
    for to_row in range(1, n_row):

        @pl.when(to_row > row)
        def _():
            pl.semaphore_signal(
                barrier, 1, device_id={"row": to_row, "col": target_col}, device_id_type=MESH
            )
    for other in others:
        pl.semaphore_signal(barrier, 1, device_id={"col": other}, device_id_type=MESH)

    earlier = jnp.clip(row - col * span, 0, span)
    pl.semaphore_wait(barrier, row + 1 - own + n_col * earlier + n_col - 1)
    for step in range(span):
        for from_col in range(n_col):
            from_row = col * span + step

            @pl.when(from_row < row)
            def _():
                pl.semaphore_signal(
                    ready.at[row],
                    1,
                    device_id={"row": from_row, "col": from_col},
                    device_id_type=MESH,
                )

    def project(weight, bias):
        offset = shift_product(in_shift[...], weight[...]) + bias[...]
        return jnp.dot(scaled, weight[...], preferred_element_type=jnp.float32) * in_spread + offset

    def edges(weight, bias):
        joined = project(weight, bias)
        edge = sigmoid(joined[:, :hidden]) * joined[:, hidden:]
        return edge.astype(jnp.bfloat16).reshape(rows, cols, hidden)

    for at in (0, 1, 2, 5, 6):
        loads[at].wait()
    values = pair[...].astype(jnp.float32).reshape(rows * cols, chans)
    center = values - jnp.mean(values, axis=1, keepdims=True)
    scaled = (center * in_gain[...]).astype(jnp.bfloat16)
    in_spread = spread_of(center)
    right_edge = edges(right_w, right_b)
    right_own[...] = right_edge

    @pl.when(target_col == col)
    def _():
        right_all[slot, col] = right_edge

    def right_copy(to_row):
        return pltpu.make_async_remote_copy(
            src_ref=right_own,
            dst_ref=right_all.at[slot, col],
            send_sem=right_send.at[to_row],
            recv_sem=right_recv.at[slot, col],
            device_id={"row": to_row, "col": target_col},
            device_id_type=MESH,
        )

    for to_row in range(n_row):
        remote = jnp.logical_or(to_row < row, jnp.logical_and(to_row == row, target_col != col))

        @pl.when(remote)
        def _():
            right_copy(to_row).start()

    for at in (3, 4):
        loads[at].wait()
    left_all[col] = edges(left_w, left_b)
    left_copies = []
    for step, other in enumerate(others):
        copy = pltpu.make_async_remote_copy(
            src_ref=left_all.at[col],
            dst_ref=left_all.at[col],
            send_sem=left_sems.at[0, step],
            recv_sem=left_sems.at[1, step],
            device_id={"col": other},
            device_id_type=MESH,
        )
        left_copies.append(copy)
        copy.start()

    for at in (7, 8, 9, 10, 11, 12):
        loads[at].wait()
    gate = sigmoid(project(gate_w, gate_b))

    for to_row in range(1, n_row):

        @pl.when(to_row > row)
        def _():
            pl.semaphore_wait(ready.at[to_row], 1)
            right_copy(to_row).start()

    out_offset = shift_product(out_shift[...], out_w[...]) + out_b[...]

    for copy in left_copies:
        copy.wait_recv()
    left = [left_all[part].astype(jnp.float32) for part in range(n_col)]
    backwards = (row > col * span).astype(jnp.int32)
    for step in range(span):
        block = step + backwards * (span - 1 - 2 * step)
        for part in range(n_col):

            @pl.when(jnp.logical_or(col * span + block != row, part != col))
            def _():
                pltpu.make_async_remote_copy(
                    src_ref=right_own,
                    dst_ref=right_all.at[block, part],
                    send_sem=right_send.at[0],
                    recv_sem=right_recv.at[block, part],
                    device_id={"row": col * span + block, "col": part},
                    device_id_type=MESH,
                ).wait_recv()

        for j in range(rows):
            right = [right_all[block, part, j].astype(jnp.float32) for part in range(n_col)]
            for i in range(rows):
                product = sum(left[part][i] * right[part] for part in range(n_col))
                product = product.reshape(cols // 8, 8, hidden).sum(axis=0)
                at = pl.multiple_of(((i * span + block) * rows + j) * 8, 8)
                partial[pl.ds(at, 8), :] = product
    n_pairs = rows * span * rows
    triangle = sum(partial[pl.ds(at, n_pairs, stride=8), :] for at in range(8))
    triangle = triangle.astype(jnp.bfloat16).astype(jnp.float32)
    center = triangle - jnp.mean(triangle, axis=1, keepdims=True)
    mixed = (center * out_gain[...]).astype(jnp.bfloat16)
    projected = jnp.dot(mixed, out_w[...], preferred_element_type=jnp.float32)
    projected = projected * spread_of(center) + out_offset
    out_ref[...] = (gate * projected).astype(jnp.bfloat16).reshape(out_ref.shape)

    for to_row in range(n_row):

        @pl.when(jnp.logical_or(to_row != row, target_col != col))
        def _():
            right_copy(to_row).wait_send()

    for copy in left_copies:
        copy.wait_send()


def kernel_plan(n_row, n_col, pair_act, *params):
    rows, cols, chans = pair_act.shape
    hidden = params[2].shape[1] // 2
    span = n_row // n_col
    operands = [pair_act] + [p.reshape(1, -1) if p.ndim == 1 else p for p in params]
    scratch = [pltpu.VMEM(o.shape, o.dtype) for o in operands]
    scratch += [
        pltpu.VMEM((rows, cols, hidden), jnp.bfloat16),
        pltpu.VMEM((span, n_col, rows, cols, hidden), jnp.bfloat16),
        pltpu.VMEM((n_col, rows, cols, hidden), jnp.bfloat16),
        pltpu.VMEM((rows * span * rows * 8, hidden), jnp.float32),
        pltpu.SemaphoreType.DMA((len(operands),)),
        pltpu.SemaphoreType.DMA((2, max(n_col - 1, 1))),
        pltpu.SemaphoreType.DMA((n_row,)),
        pltpu.SemaphoreType.DMA((span, n_col)),
        pltpu.SemaphoreType.REGULAR((n_row,)),
    ]
    return pl.pallas_call(
        functools.partial(kernel, n_row, n_col),
        out_shape=pltpu.VMEM((rows, cols, chans), jnp.bfloat16),
        in_specs=[pl.BlockSpec(memory_space=pl.ANY)] * len(operands),
        out_specs=pl.BlockSpec(memory_space=pltpu.VMEM),
        scratch_shapes=scratch,
        compiler_params=pltpu.CompilerParams(collective_id=0, has_side_effects=True),
    )(*operands)


def fits(n_row, n_col, rows, cols, hidden):
    gathered = n_row * rows * cols * hidden * 2
    square = rows * n_row == cols * n_col
    return square and n_row % n_col == 0 and cols % 8 == 0 and gathered <= KERNEL_BYTES


def solution(mesh):
    n_row, n_col = mesh.shape["row"], mesh.shape["col"]

    def per_device(pair_act, *params):
        rows, cols, _ = pair_act.shape
        if fits(n_row, n_col, rows, cols, params[2].shape[1] // 2):
            return kernel_plan(n_row, n_col, pair_act, *params)
        return collective_plan(pair_act, *params)

    spec = P(("groups", "row"), "col", None)
    return jax.shard_map(
        per_device, mesh=mesh, in_specs=(spec,) + (P(),) * 12, out_specs=spec, check_vma=False
    )
```
